128 devices in a mesh: gz: 4 (over x_lo, core), gy: 32 (over y, x_hi, z).
Axes of the slice: x: 4 (x_hi: 2, x_lo: 2; x = x_hi * 2 + x_lo), y: 4, z: 4, core: 2. Of those that a mesh axis runs over, the one named last changes fastest.
Arguments:
- distance: float32 [256, 512, 1024], P('gz', 'gy'), may hold values from 0 to 2
- parent: int32 [256, 512, 1024], P('gz', 'gy'), may hold values from 0 to 4095, as said below
- removed: int32 [4096], replicated, may hold values from 0 to 1
- occupied: int32 [256, 512, 1024], P('gz', 'gy'), may hold values 0 or 1
Outputs:
- lowered: float32 [256, 512, 1024], P('gz', 'gy')
- cleared_share: float32 [], replicated
The draws below stay inside these ranges and needn't reach their ends.
Inputs may be any that keep to these rules, and one draw needn't show every extreme that they name: `parent`: an obstacle id.
All inputs are finite; a program needn't handle non-finite values. No bound on the sum of `occupied` on one device may be relied on, other than what follows from the above.
Results may differ from the reference program's by a relative error of at most 0.0003.
Values sent between devices are 32-bit elements; how exact they have to be, the bound alone decides.
A program may use at most 64 MiB of HBM per device.

```python
import jax
import jax.numpy as jnp
from jax import lax

OBJS = 4096
NZ = 256
NY = 512
NX = 1024


def draw_parent(key, part):
    zcoord = lax.broadcasted_iota(jnp.int32, (NZ, NY, NX), 0)
    ycoord = lax.broadcasted_iota(jnp.int32, (NZ, NY, NX), 1)
    half = OBJS // 2
    base = (zcoord * NY + ycoord * NZ) * half // (2 * NZ * NY)
    return (base + jax.random.randint(key, (NZ, NY, NX), 0, half, dtype=jnp.int32)).astype(jnp.int32)


def draw_removed(key, part):
    ident = lax.iota(jnp.int32, OBJS)
    level = 30 * ident // OBJS
    rolled = jax.random.randint(key, (OBJS,), 0, 1000, dtype=jnp.int32)
    return (rolled < 30 + level * level).astype(jnp.int32)


def place_ends(array, rng, smallest, top_value):
    longest = array.shape.index(max(array.shape))
    spots = []
    for shift in (0, 1):
        where = [jax.random.randint(jax.random.fold_in(rng, axis), (), 0, length) for axis, length in enumerate(array.shape)]
        where[longest] = (where[longest] + shift) % array.shape[longest]
        spots.append(tuple(where))
    return array.at[spots[0]].set(smallest).at[spots[1]].set(top_value)


def level_of(stream_key, shape, split, smallest, high):
    factor_of, own = 1.0, jax.random.fold_in(stream_key, 6)
    for axis_at, shards_of in split:
        heights = jnp.exp(jax.random.uniform(jax.random.fold_in(own, axis_at), (shards_of,), jnp.float32, smallest / len(split), high / len(split)))
        factor_of = factor_of * jnp.repeat(heights, shape[axis_at] // shards_of).reshape([-1 if axis == axis_at else 1 for axis in range(len(shape))])
    return factor_of


def setup_inputs(seed: int = 0) -> dict:
    keys = jax.random.split(jax.random.key(seed), 5)
    return {
        "distance": jnp.clip(2.0 * jax.random.uniform(keys[0], (NZ, NY, NX), jnp.float32) ** level_of(keys[0], (NZ, NY, NX), ((0, 4), (1, 32)), -0.2, 0.2), 0.0, 2.0),
        "parent": draw_parent(jax.random.fold_in(keys[4], 71), 0),
        "removed": draw_removed(jax.random.fold_in(keys[4], 71), 0),
        "occupied": place_ends((jax.random.randint(keys[3], (NZ, NY, NX), 0, 16) < 1).astype(jnp.int32), jax.random.fold_in(keys[3], 1), 0, 1),
    }


FAR = 1.0e6
VOXEL = 0.1
TRUNC = 2.0


def sweep(field):
    far_plane = jnp.full((1,) + field.shape[1:], FAR, field.dtype)
    zpad = jnp.concatenate([far_plane, field, far_plane], 0)
    nearest = jnp.minimum(zpad[2:], zpad[:-2])
    ypad = jnp.concatenate([field[:, -1:], field, field[:, :1]], 1)
    nearest = jnp.minimum(nearest, jnp.minimum(ypad[:, 2:], ypad[:, :-2]))
    far_col = jnp.full(field.shape[:2] + (1,), FAR, field.dtype)
    right = jnp.concatenate([field[:, :, 1:], far_col], 2)
    left = jnp.concatenate([far_col, field[:, :, :-1]], 2)
    nearest = jnp.minimum(nearest, jnp.minimum(left, right))
    return jnp.minimum(field, nearest + VOXEL)


def reference(distance, parent, removed, occupied):
    flagged = jnp.take(removed, parent.astype(jnp.int32), axis=0)
    cleared = ((flagged == 1) & (occupied == 0)).astype(jnp.int32)
    raised = jnp.where(occupied == 1, jnp.zeros_like(distance), jnp.where(cleared == 1, jnp.full_like(distance, TRUNC), distance))
    lowered = sweep(sweep(raised))
    count = jnp.sum(cleared)
    total = distance.shape[0] * distance.shape[1] * distance.shape[2]
    share = count.astype(jnp.float32) * jnp.float32(100.0 / total)
    return lowered, share
```

```python
import functools

import jax
import jax.numpy as jnp
from jax import lax
from jax.experimental import pallas as pl
from jax.experimental.pallas import tpu as pltpu
from jax.sharding import PartitionSpec as P

MESH = pl.DeviceIdType.MESH
FAR = 1000000.0
VOXEL = 0.1
TRUNC = 2.0
Z, Y, X = 64, 16, 1024
XT = X // 128
PR = 24
RR = (Z + 2) * PR
CH = 8
NC = Z // CH
NGZ, NGY = 4, 32
SPLIT = (0,) + tuple(CH * c + CH + 1 for c in range(NC - 1)) + (Z,)


def lane_shifts(tiles, lane):
    far = jnp.full((8, 128), FAR, jnp.float32)
    up = [pltpu.roll(t, 127, 1) for t in tiles] + [far]
    down = [far] + [pltpu.roll(t, 1, 1) for t in tiles]
    right = [jnp.where(lane == 127, up[i + 1], up[i]) for i in range(len(tiles))]
    left = [jnp.where(lane == 0, down[i], down[i + 1]) for i in range(len(tiles))]
    return [jnp.minimum(a, b) for a, b in zip(right, left)]


def row(zp, y):
    return zp * PR + 8 + y


def kernel(
    dist_hbm, par_hbm, occ_hbm, rem_ref, out, share_ref,
    dist, par, occ, field, once, snd, hal, zhal, csnd, chal, tally, theirs,
    in_sem, ys_sem, yr_sem, zs_sem, zr_sem, cs_sem, cr_sem, ts_sem, tr_sem,
):
    gz, gy = lax.axis_index("gz"), lax.axis_index("gy")
    seg, zc = gy // 4, gy % 4
    lo, hi = (gz, (gy + NGY - 1) % NGY), (gz, (gy + 1) % NGY)
    below, above = (gz + NGZ - 1) % NGZ, (gz + 1) % NGZ
    diag = [[(g, t[1]) for t in (lo, hi)] for g in (below, above)]
    stage = [
        [(gz, seg * 4 + (zc + r) % 4) for r in range(1, 4)],
        [(gz, ((seg + r) % 8) * 4 + zc) for r in range(1, 8)],
        [((gz + r) % 4, gy) for r in range(1, 4)],
    ]
    first_slot = (0, 3, 10)
    friends = [lo, hi, (below, gy), (above, gy)] + diag[0] + diag[1] + stage[0] + stage[1] + stage[2]

    barrier = pltpu.get_barrier_semaphore()
    for friend in friends:
        pl.semaphore_signal(barrier, inc=1, device_id=friend, device_id_type=MESH)

    def fetch(c):
        a, n = SPLIT[c], SPLIT[c + 1] - SPLIT[c]
        return [
            pltpu.make_async_copy(src.at[pl.ds(a, n)], dst.at[pl.ds(a, n)], in_sem.at[i, c])
            for i, (src, dst) in enumerate(((dist_hbm, dist), (par_hbm, par), (occ_hbm, occ)))
        ]

    for c in range(NC):
        for copy in fetch(c):
            copy.start()

    lane = lax.broadcasted_iota(jnp.int32, (8, 128), 1)
    far_tile = jnp.full((8, 128), FAR, jnp.float32)

    bits = rem_ref[...] << lax.broadcasted_iota(jnp.int32, (32, 128), 0)
    words = jnp.broadcast_to(jnp.sum(bits, axis=0, keepdims=True), (8, 128))

    def pad_plane(zp, _):
        for xt in range(XT):
            base = pl.multiple_of(xt * RR + zp * PR, 8)
            field[pl.ds(base, 8), :] = far_tile
            once[pl.ds(base, 8), :] = far_tile
        return 0

    lax.fori_loop(0, Z + 2, pad_plane, 0)
    for xt in range(XT):
        for zp in (0, Z + 1):
            for half in (8, 16):
                field[pl.ds(xt * RR + zp * PR + half, 8), :] = far_tile
                once[pl.ds(xt * RR + zp * PR + half, 8), :] = far_tile
    for side in range(2):
        for plane in range(2):
            for xt in range(XT):
                zhal[side, plane, xt, pl.ds(0, 8), :] = far_tile
                zhal[side, plane, xt, pl.ds(24, 8), :] = far_tile

    def raise_plane(z, acc):
        for yt in range(2):
            for xt in range(XT):
                at = (z, pl.ds(yt * 8, 8), pl.ds(xt * 128, 128))
                ids, busy = par[at], occ[at]
                word = jnp.take_along_axis(words, ids & 127, axis=1, mode="promise_in_bounds")
                gone = lax.shift_right_logical(word, ids >> 7) & (1 - busy)
                raised = jnp.where(gone == 1, TRUNC, dist[at])
                raised = jnp.where(busy == 1, 0.0, raised)
                field[pl.ds(pl.multiple_of(xt * RR + (z + 1) * PR + 8 + yt * 8, 8), 8), :] = raised
                acc = acc + gone
        return acc

    def pack(c):
        first = c * CH + 1
        for side in range(2):
            y1, y2 = ((0, 1), (15, 14))[side]

            def rows(zp, y, xt):
                return field[pl.ds(xt * RR + row(zp, y), CH, stride=PR), :]

            near = [rows(first, y1, xt) for xt in range(XT)]
            around = lane_shifts(near, lane)
            for xt in range(XT):
                two = jnp.minimum(around[xt], rows(first, y2, xt))
                two = jnp.minimum(two, jnp.minimum(rows(first - 1, y1, xt), rows(first + 1, y1, xt)))
                snd[side, c, 0, xt] = jnp.minimum(near[xt] + VOXEL, two + VOXEL + VOXEL)
                snd[side, c, 1, xt] = near[xt] + VOXEL + VOXEL

    def y_copy(side, c):
        return pltpu.make_async_remote_copy(
            src_ref=snd.at[side, c], dst_ref=hal.at[1 - side, c],
            send_sem=ys_sem.at[side, c], recv_sem=yr_sem.at[1 - side, c],
            device_id=(lo, hi)[side], device_id_type=MESH,
        )

    def y_send(c):
        for side in (1, 0):
            y_copy(side, c).start()

    def z_copy(side, plane):
        zp = ((1, 2), (Z, Z - 1))[side][plane]
        return [
            pltpu.make_async_remote_copy(
                src_ref=field.at[pl.ds(xt * RR + row(zp, 0), 16)],
                dst_ref=zhal.at[1 - side, plane, xt, pl.ds(8, 16)],
                send_sem=zs_sem.at[side, plane, xt], recv_sem=zr_sem.at[1 - side, plane, xt],
                device_id=((below, gy), (above, gy))[side], device_id_type=MESH,
            )
            for xt in range(XT)
        ]

    def corner_copy(zs, ys):
        return pltpu.make_async_remote_copy(
            src_ref=csnd.at[zs, ys], dst_ref=chal.at[1 - zs, 1 - ys],
            send_sem=cs_sem.at[zs, ys], recv_sem=cr_sem.at[1 - zs, 1 - ys],
            device_id=diag[zs][ys], device_id_type=MESH,
        )

    def z_copies(side):
        return z_copy(side, 0) + z_copy(side, 1) + [corner_copy(side, 0), corner_copy(side, 1)]

    has = (gz > 0, gz < NGZ - 1)

    def z_send(side):
        for ys in range(2):
            csnd[side, ys] = field[pl.ds(row((1, Z)[side], (0, Y - 1)[ys]), 8, stride=RR), :]

        @pl.when(has[side])
        def _():
            for copy in z_copies(side):
                copy.start()

    def tally_copies(s):
        return [
            pltpu.make_async_remote_copy(
                src_ref=tally.at[s], dst_ref=theirs.at[first_slot[s] + r],
                send_sem=ts_sem.at[first_slot[s] + r], recv_sem=tr_sem.at[first_slot[s] + r],
                device_id=peer, device_id_type=MESH,
            )
            for r, peer in enumerate(stage[s])
        ]

    def tally_send(s, value):
        tally[s] = value
        for copy in tally_copies(s):
            copy.start()

    def tally_wait(s, value):
        for r, copy in enumerate(tally_copies(s)):
            copy.wait()
            value = value + theirs[first_slot[s] + r]
        return value

    def sweep_chunk(src, store, c):
        def plane(z, _):
            for yt in range(2):
                base = [xt * RR + (z + 1) * PR + 8 + yt * 8 for xt in range(XT)]
                here = [src[pl.ds(pl.multiple_of(b, 8), 8), :] for b in base]
                around = lane_shifts(here, lane)
                for xt in range(XT):
                    b = base[xt]
                    m = jnp.minimum(
                        src[pl.ds(pl.multiple_of(b - PR, 8), 8), :],
                        src[pl.ds(pl.multiple_of(b + PR, 8), 8), :],
                    )
                    m = jnp.minimum(m, jnp.minimum(src[pl.ds(b - 1, 8), :], src[pl.ds(b + 1, 8), :]))
                    m = jnp.minimum(m, around[xt])
                    store(z, yt, xt, jnp.minimum(here[xt], m + VOXEL))
            return 0

        lax.fori_loop(c * CH, (c + 1) * CH, plane, 0)

    def store_once(z, yt, xt, value):
        once[pl.ds(pl.multiple_of(xt * RR + (z + 1) * PR + 8 + yt * 8, 8), 8), :] = value

    def out_row(z, yt, xt):
        return ((z * 2 + yt) * XT + xt) * 8

    def store_out(z, yt, xt, value):
        out[pl.ds(pl.multiple_of(out_row(z, yt, xt), 8), 8), :] = value

    acc = jnp.zeros((8, 128), jnp.int32)
    for c in range(NC):
        for copy in fetch(c):
            copy.wait()
        acc = lax.fori_loop(SPLIT[c], SPLIT[c + 1], raise_plane, acc)
        pack(c)
        if c == 3:
            pl.semaphore_wait(barrier, len(friends))
            y_send(0)
            z_send(0)
        if c == 5:
            y_send(1)
    z_send(1)
    tally_send(0, acc)
    y_send(2)
    y_send(3)

    for c in range(NC):
        sweep_chunk(field, store_once, c)
        if c in (1, 3, 5, 7):
            y_send(4 + c // 2)
        if c == 5:
            acc = tally_wait(0, acc)
            tally_send(1, acc)
    for c in range(NC):
        sweep_chunk(once, store_out, c)
        if c == 3:
            acc = tally_wait(1, acc)
            tally_send(2, acc)

    for side in range(2):
        z0, z1 = ((0, 1), (Z - 1, Z - 2))[side]

        @pl.when(has[side])
        def _():
            for sent, came in zip(z_copies(side), z_copies(1 - side)):
                sent.wait_send()
                came.wait_recv()
            for yt in range(2):
                near = [zhal[side, 0, xt, pl.ds(8 + yt * 8, 8), :] for xt in range(XT)]
                around = lane_shifts(near, lane)
                for xt in range(XT):
                    two = jnp.minimum(around[xt], zhal[side, 1, xt, pl.ds(8 + yt * 8, 8), :])
                    two = jnp.minimum(
                        two,
                        jnp.minimum(
                            zhal[side, 0, xt, pl.ds(7 + yt * 8, 8), :],
                            zhal[side, 0, xt, pl.ds(9 + yt * 8, 8), :],
                        ),
                    )
                    add0 = jnp.minimum(near[xt] + VOXEL, two + VOXEL + VOXEL)
                    at0 = pl.ds(out_row(z0, yt, xt), 8)
                    out[at0, :] = jnp.minimum(out[at0, :], add0)
                    at1 = pl.ds(out_row(z1, yt, xt), 8)
                    out[at1, :] = jnp.minimum(out[at1, :], near[xt] + VOXEL + VOXEL)
            for ys in range(2):
                at = pl.ds(out_row(z0, ys, 0) + (0, 7)[ys], 8, stride=8)
                out[at, :] = jnp.minimum(out[at, :], chal[side, ys] + VOXEL + VOXEL)

    acc = tally_wait(2, acc)
    count = jnp.sum(acc)
    share_ref[0, 0] = count.astype(jnp.float32) * jnp.float32(100.0 / (NGZ * Z * NGY * Y * X))

    for c in range(NC):
        for side in range(2):
            y_copy(1 - side, c).wait()
            for which in range(2):
                y = ((0, 1), (15, 14))[side][which]
                for xt in range(XT):
                    at = pl.ds(out_row(c * CH, y // 8, xt) + y % 8, CH, stride=2 * XT * 8)
                    out[at, :] = jnp.minimum(out[at, :], hal[side, c, which, xt])


def on_device(distance, parent, removed, occupied):
    hbm = pl.BlockSpec(memory_space=pltpu.HBM)
    vmem = pl.BlockSpec(memory_space=pltpu.VMEM)
    dma = pltpu.SemaphoreType.DMA
    flat, share = pl.pallas_call(
        kernel,
        out_shape=(
            jax.ShapeDtypeStruct((Z * Y * XT, 128), jnp.float32),
            jax.ShapeDtypeStruct((1, 1), jnp.float32),
        ),
        in_specs=[hbm, hbm, hbm, vmem],
        out_specs=(vmem, pl.BlockSpec(memory_space=pltpu.SMEM)),
        scratch_shapes=[
            pltpu.VMEM((Z, Y, X), jnp.float32),
            pltpu.VMEM((Z, Y, X), jnp.int32),
            pltpu.VMEM((Z, Y, X), jnp.int32),
            pltpu.VMEM((XT * RR, 128), jnp.float32),
            pltpu.VMEM((XT * RR, 128), jnp.float32),
            pltpu.VMEM((2, NC, 2, XT, CH, 128), jnp.float32),
            pltpu.VMEM((2, NC, 2, XT, CH, 128), jnp.float32),
            pltpu.VMEM((2, 2, XT, 32, 128), jnp.float32),
            pltpu.VMEM((2, 2, 8, 128), jnp.float32),
            pltpu.VMEM((2, 2, 8, 128), jnp.float32),
            pltpu.VMEM((3, 8, 128), jnp.int32),
            pltpu.VMEM((13, 8, 128), jnp.int32),
            dma((3, NC)),
            dma((2, NC)),
            dma((2, NC)),
            dma((2, 2, XT)),
            dma((2, 2, XT)),
            dma((2, 2)),
            dma((2, 2)),
            dma((13,)),
            dma((13,)),
        ],
        compiler_params=pltpu.CompilerParams(
            collective_id=0, has_side_effects=True, vmem_limit_bytes=57 * 2**20
        ),
    )(distance, parent, occupied, removed.reshape(32, 128))
    lowered = flat.reshape(Z, 2, XT, 8, 128).transpose(0, 1, 3, 2, 4).reshape(Z, Y, X)
    return lowered, share.reshape(())


def solution(mesh):
    block = P("gz", "gy", None)
    return jax.shard_map(
        on_device, mesh=mesh, in_specs=(block, block, P(), block), out_specs=(block, P()), check_vma=False
    )
```

```python
import functools

import jax
import jax.numpy as jnp
from jax import lax
from jax.experimental import pallas as pl
from jax.experimental.pallas import tpu as pltpu
from jax.sharding import PartitionSpec as P

MESH = pl.DeviceIdType.MESH
FAR = 1000000.0
VOXEL = 0.1
TRUNC = 2.0
Z, Y, X = 64, 16, 1024
XT = X // 128
PR = 24
RR = (Z + 2) * PR
CH = 8
NC = Z // CH
NGZ, NGY = 4, 32
WAIT_AT = 2
EARLY = ((), (), (0, 1), (2,), (), (), (), (3,))
UNITS = (0, 7, 1, 2, 3, 4, 5, 6)
READY = ((0,), (), (1,), (2,), (3,), (4,), (5,), (6, 7))
SPLIT = (0,) + tuple(CH * c + CH + 1 for c in range(NC - 1)) + (Z,)


def lane_shifts(tiles, lane):
    far = jnp.full((8, 128), FAR, jnp.float32)
    up = [pltpu.roll(t, 127, 1) for t in tiles] + [far]
    down = [far] + [pltpu.roll(t, 1, 1) for t in tiles]
    right = [jnp.where(lane == 127, up[i + 1], up[i]) for i in range(len(tiles))]
    left = [jnp.where(lane == 0, down[i], down[i + 1]) for i in range(len(tiles))]
    return [jnp.minimum(a, b) for a, b in zip(right, left)]


def lane_gather(table, index):
    dims = lax.GatherDimensionNumbers(
        offset_dims=(),
        collapsed_slice_dims=(1,),
        start_index_map=(1,),
        operand_batching_dims=(0,),
        start_indices_batching_dims=(0,),
    )
    mode = lax.GatherScatterMode.PROMISE_IN_BOUNDS
    return lax.gather(table, index[..., None], dims, (1, 1), mode=mode)


def row(zp, y):
    return zp * PR + 8 + y


def kernel(
    dist_hbm, par_hbm, occ_hbm, rem_hbm, out, share_ref,
    dist, par, occ, field, once, snd, hal, zhal, csnd, chal, tally, theirs, rem,
    rem_sem, in_sem, ys_sem, yr_sem, zs_sem, zr_sem, cs_sem, cr_sem, ts_sem, tr_sem,
):
    gz, gy = lax.axis_index("gz"), lax.axis_index("gy")
    zc = gy % 4
    lo, hi = (gz, (gy + NGY - 1) % NGY), (gz, (gy + 1) % NGY)
    below, above = (gz + NGZ - 1) % NGZ, (gz + 1) % NGZ
    diag = [[(g, t[1]) for t in (lo, hi)] for g in (below, above)]
    seg = gy // 4
    stage = [
        [(gz, seg * 4 + (zc + r) % 4) for r in range(1, 4)],
        [(gz, ((seg + r) % 8) * 4 + zc) for r in range(1, 8)],
        [((gz + r) % 4, gy) for r in range(1, 4)],
    ]
    first_slot = (0, 3, 10)
    friends = [lo, hi, (below, gy), (above, gy)] + diag[0] + diag[1] + stage[0] + stage[1] + stage[2]

    barrier = pltpu.get_barrier_semaphore()
    for friend in friends:
        pl.semaphore_signal(barrier, inc=1, device_id=friend, device_id_type=MESH)

    fetch_removed = pltpu.make_async_copy(rem_hbm, rem, rem_sem)
    fetch_removed.start()

    def fetch(c):
        a, n = SPLIT[c], SPLIT[c + 1] - SPLIT[c]
        return [
            pltpu.make_async_copy(src.at[pl.ds(a, n)], dst.at[pl.ds(a, n)], in_sem.at[i, c])
            for i, (src, dst) in enumerate(((dist_hbm, dist), (par_hbm, par), (occ_hbm, occ)))
        ]

    for c in UNITS:
        for copy in fetch(c):
            copy.start()

    lane = lax.broadcasted_iota(jnp.int32, (8, 128), 1)
    far_tile = jnp.full((8, 128), FAR, jnp.float32)

    fetch_removed.wait()
    bits = rem[...] << lax.broadcasted_iota(jnp.int32, (32, 128), 0)
    words = jnp.broadcast_to(jnp.sum(bits, axis=0, keepdims=True), (8, 128))

    def pad_plane(zp, _):
        for xt in range(XT):
            base = pl.multiple_of(xt * RR + zp * PR, 8)
            field[pl.ds(base, 8), :] = far_tile
            once[pl.ds(base, 8), :] = far_tile
        return 0

    lax.fori_loop(0, Z + 2, pad_plane, 0)
    for xt in range(XT):
        for zp in (0, Z + 1):
            for half in (8, 16):
                field[pl.ds(xt * RR + zp * PR + half, 8), :] = far_tile
                once[pl.ds(xt * RR + zp * PR + half, 8), :] = far_tile
    for side in range(2):
        for plane in range(2):
            for xt in range(XT):
                zhal[side, plane, xt, pl.ds(0, 8), :] = far_tile
                zhal[side, plane, xt, pl.ds(24, 8), :] = far_tile

    def raise_plane(z, acc):
        for yt in range(2):
            for xt in range(XT):
                at = (z, pl.ds(yt * 8, 8), pl.ds(xt * 128, 128))
                ids, busy = par[at], occ[at]
                word = lane_gather(words, ids & 127)
                gone = lax.shift_right_logical(word, ids >> 7) & (1 - busy)
                raised = jnp.where(gone == 1, TRUNC, dist[at])
                raised = jnp.where(busy == 1, 0.0, raised)
                field[pl.ds(pl.multiple_of(xt * RR + (z + 1) * PR + 8 + yt * 8, 8), 8), :] = raised
                acc = acc + gone
        return acc

    def pack(c):
        first = c * CH + 1
        for side in range(2):
            y1, y2 = ((0, 1), (15, 14))[side]

            def rows(zp, y, xt):
                return field[pl.ds(xt * RR + row(zp, y), CH, stride=PR), :]

            near = [rows(first, y1, xt) for xt in range(XT)]
            around = lane_shifts(near, lane)
            for xt in range(XT):
                two = jnp.minimum(around[xt], rows(first, y2, xt))
                two = jnp.minimum(two, jnp.minimum(rows(first - 1, y1, xt), rows(first + 1, y1, xt)))
                snd[side, c, 0, xt] = jnp.minimum(near[xt] + VOXEL, two + VOXEL + VOXEL)
                snd[side, c, 1, xt] = near[xt] + VOXEL + VOXEL

    def y_copy(side, c):
        return pltpu.make_async_remote_copy(
            src_ref=snd.at[side, c], dst_ref=hal.at[1 - side, c],
            send_sem=ys_sem.at[side, c], recv_sem=yr_sem.at[1 - side, c],
            device_id=(lo, hi)[side], device_id_type=MESH,
        )

    def y_send(c):
        for side in (1, 0):
            y_copy(side, c).start()

    def z_copy(side, plane):
        zp = ((1, 2), (Z, Z - 1))[side][plane]
        return [
            pltpu.make_async_remote_copy(
                src_ref=field.at[pl.ds(xt * RR + row(zp, 0), 16)],
                dst_ref=zhal.at[1 - side, plane, xt, pl.ds(8, 16)],
                send_sem=zs_sem.at[side, plane, xt], recv_sem=zr_sem.at[1 - side, plane, xt],
                device_id=((below, gy), (above, gy))[side], device_id_type=MESH,
            )
            for xt in range(XT)
        ]

    def corner_copy(zs, ys):
        return pltpu.make_async_remote_copy(
            src_ref=csnd.at[zs, ys], dst_ref=chal.at[1 - zs, 1 - ys],
            send_sem=cs_sem.at[zs, ys], recv_sem=cr_sem.at[1 - zs, 1 - ys],
            device_id=diag[zs][ys], device_id_type=MESH,
        )

    def z_copies(side):
        return z_copy(side, 0) + z_copy(side, 1)

    def corners(side):
        return [corner_copy(side, 0), corner_copy(side, 1)]

    has = (gz > 0, gz < NGZ - 1)

    def z_send(side):
        @pl.when(has[side])
        def _():
            for copy in z_copies(side):
                copy.start()

    def corner_send(side):
        @pl.when(has[side])
        def _():
            for copy in corners(side):
                copy.start()

    def tally_copies(s):
        return [
            pltpu.make_async_remote_copy(
                src_ref=tally.at[s], dst_ref=theirs.at[first_slot[s] + r],
                send_sem=ts_sem.at[first_slot[s] + r], recv_sem=tr_sem.at[first_slot[s] + r],
                device_id=peer, device_id_type=MESH,
            )
            for r, peer in enumerate(stage[s])
        ]

    def tally_send(s, value):
        tally[s] = value
        for copy in tally_copies(s):
            copy.start()

    def tally_wait(s, value):
        for r, copy in enumerate(tally_copies(s)):
            copy.wait()
            value = value + theirs[first_slot[s] + r]
        return value

    def sweep_chunk(src, store, c):
        def plane(z, _):
            for yt in range(2):
                base = [xt * RR + (z + 1) * PR + 8 + yt * 8 for xt in range(XT)]
                here = [src[pl.ds(pl.multiple_of(b, 8), 8), :] for b in base]
                around = lane_shifts(here, lane)
                for xt in range(XT):
                    b = base[xt]
                    m = jnp.minimum(
                        src[pl.ds(pl.multiple_of(b - PR, 8), 8), :],
                        src[pl.ds(pl.multiple_of(b + PR, 8), 8), :],
                    )
                    m = jnp.minimum(m, jnp.minimum(src[pl.ds(b - 1, 8), :], src[pl.ds(b + 1, 8), :]))
                    m = jnp.minimum(m, around[xt])
                    store(z, yt, xt, jnp.minimum(here[xt], m + VOXEL))
            return 0

        lax.fori_loop(c * CH, (c + 1) * CH, plane, 0, unroll=8)

    def store_once(z, yt, xt, value):
        once[pl.ds(pl.multiple_of(xt * RR + (z + 1) * PR + 8 + yt * 8, 8), 8), :] = value

    def out_row(z, yt, xt):
        return ((z * 2 + yt) * XT + xt) * 8

    def store_out(z, yt, xt, value):
        out[pl.ds(pl.multiple_of(out_row(z, yt, xt), 8), 8), :] = value

    acc = jnp.zeros((8, 128), jnp.int32)
    for turn, u in enumerate(UNITS):
        for copy in fetch(u):
            copy.wait()
        acc = lax.fori_loop(SPLIT[u], SPLIT[u + 1], raise_plane, acc, unroll=8)
        if turn == 1:
            for zs in range(2):
                for ys in range(2):
                    csnd[zs, ys] = field[pl.ds(row((1, Z)[zs], (0, Y - 1)[ys]), 8, stride=RR), :]
        for c in READY[turn]:
            pack(c)
        if turn == WAIT_AT:
            pl.semaphore_wait(barrier, len(friends))
            corner_send(0)
            corner_send(1)
        if turn >= WAIT_AT:
            for c in EARLY[turn]:
                y_send(c)
    tally_send(0, acc)
    y_send(4)

    for c in range(NC):
        sweep_chunk(field, store_once, c)
        if c == 5:
            y_send(5)
    for c in range(NC):
        sweep_chunk(once, store_out, c)
        if c == 2:
            y_send(6)
        if c == 6:
            y_send(7)
            z_send(0)
            z_send(1)
    acc = tally_wait(0, acc)
    tally_send(1, acc)

    for side in range(2):
        z0, z1 = ((0, 1), (Z - 1, Z - 2))[side]

        @pl.when(has[side])
        def _():
            for sent, came in zip(z_copies(side) + corners(side), z_copies(1 - side) + corners(1 - side)):
                sent.wait_send()
                came.wait_recv()
            for yt in range(2):
                near = [zhal[side, 0, xt, pl.ds(8 + yt * 8, 8), :] for xt in range(XT)]
                around = lane_shifts(near, lane)
                for xt in range(XT):
                    two = jnp.minimum(around[xt], zhal[side, 1, xt, pl.ds(8 + yt * 8, 8), :])
                    two = jnp.minimum(
                        two,
                        jnp.minimum(
                            zhal[side, 0, xt, pl.ds(7 + yt * 8, 8), :],
                            zhal[side, 0, xt, pl.ds(9 + yt * 8, 8), :],
                        ),
                    )
                    add0 = jnp.minimum(near[xt] + VOXEL, two + VOXEL + VOXEL)
                    at0 = pl.ds(out_row(z0, yt, xt), 8)
                    out[at0, :] = jnp.minimum(out[at0, :], add0)
                    at1 = pl.ds(out_row(z1, yt, xt), 8)
                    out[at1, :] = jnp.minimum(out[at1, :], near[xt] + VOXEL + VOXEL)
            for ys in range(2):
                at = pl.ds(out_row(z0, ys, 0) + (0, 7)[ys], 8, stride=8)
                out[at, :] = jnp.minimum(out[at, :], chal[side, ys] + VOXEL + VOXEL)

    for c in range(NC):
        for side in range(2):
            y_copy(1 - side, c).wait()
            for which in range(2):
                y = ((0, 1), (15, 14))[side][which]
                for xt in range(XT):
                    at = pl.ds(out_row(c * CH, y // 8, xt) + y % 8, CH, stride=2 * XT * 8)
                    out[at, :] = jnp.minimum(out[at, :], hal[side, c, which, xt])
        if c == 5:
            acc = tally_wait(1, acc)
            tally_send(2, acc)

    acc = tally_wait(2, acc)
    count = jnp.sum(acc)
    share_ref[0, 0] = count.astype(jnp.float32) * jnp.float32(100.0 / (NGZ * Z * NGY * Y * X))


def on_device(distance, parent, removed, occupied):
    hbm = pl.BlockSpec(memory_space=pltpu.HBM)
    vmem = pl.BlockSpec(memory_space=pltpu.VMEM)
    dma = pltpu.SemaphoreType.DMA
    flat, share = pl.pallas_call(
        kernel,
        out_shape=(
            jax.ShapeDtypeStruct((Z * Y * XT, 128), jnp.float32),
            jax.ShapeDtypeStruct((1, 1), jnp.float32),
        ),
        in_specs=[hbm, hbm, hbm, hbm],
        out_specs=(vmem, pl.BlockSpec(memory_space=pltpu.SMEM)),
        scratch_shapes=[
            pltpu.VMEM((Z, Y, X), jnp.float32),
            pltpu.VMEM((Z, Y, X), jnp.int32),
            pltpu.VMEM((Z, Y, X), jnp.int32),
            pltpu.VMEM((XT * RR, 128), jnp.float32),
            pltpu.VMEM((XT * RR, 128), jnp.float32),
            pltpu.VMEM((2, NC, 2, XT, CH, 128), jnp.float32),
            pltpu.VMEM((2, NC, 2, XT, CH, 128), jnp.float32),
            pltpu.VMEM((2, 2, XT, 32, 128), jnp.float32),
            pltpu.VMEM((2, 2, 8, 128), jnp.float32),
            pltpu.VMEM((2, 2, 8, 128), jnp.float32),
            pltpu.VMEM((3, 8, 128), jnp.int32),
            pltpu.VMEM((13, 8, 128), jnp.int32),
            pltpu.VMEM((32, 128), jnp.int32),
            dma,
            dma((3, NC)),
            dma((2, NC)),
            dma((2, NC)),
            dma((2, 2, XT)),
            dma((2, 2, XT)),
            dma((2, 2)),
            dma((2, 2)),
            dma((13,)),
            dma((13,)),
        ],
        compiler_params=pltpu.CompilerParams(
            collective_id=0, has_side_effects=True, vmem_limit_bytes=48 * 2**20
        ),
    )(distance, parent, occupied, removed.reshape(32, 128))
    lowered = flat.reshape(Z, 2, XT, 8, 128).transpose(0, 1, 3, 2, 4).reshape(Z, Y, X)
    return lowered, share.reshape(())


def solution(mesh):
    block = P("gz", "gy", None)
    return jax.shard_map(
        on_device, mesh=mesh, in_specs=(block, block, P(), block), out_specs=(block, P()), check_vma=False
    )
```

```python
import functools

import jax
import jax.numpy as jnp
from jax import lax
from jax.experimental import pallas as pl
from jax.experimental.pallas import tpu as pltpu
from jax.sharding import PartitionSpec as P

MESH = pl.DeviceIdType.MESH
FAR = 1000000.0
VOXEL = 0.1
TRUNC = 2.0
Z, Y, X = 64, 16, 1024
XT = X // 128
PR = 24
RR = (Z + 2) * PR
CH = 8
NC = Z // CH
NGZ, NGY = 4, 32
WAIT_AT = 1
UNITS = (0, 7, 6, 1, 2, 3, 4, 5)
READY = ((0,), (), (7,), (1,), (2,), (3,), (4,), (5, 6))
EARLY = ((), (0,), (7,), (1,), (2,), (), (), ())
ORDER = (0, 7, 1, 2, 3, 4, 5, 6)
SPLIT = (0,) + tuple(CH * c + CH + 1 for c in range(NC - 1)) + (Z,)


def lane_shifts(tiles, lane):
    far = jnp.full((8, 128), FAR, jnp.float32)
    up = [pltpu.roll(t, 127, 1) for t in tiles] + [far]
    down = [far] + [pltpu.roll(t, 1, 1) for t in tiles]
    right = [jnp.where(lane == 127, up[i + 1], up[i]) for i in range(len(tiles))]
    left = [jnp.where(lane == 0, down[i], down[i + 1]) for i in range(len(tiles))]
    return [jnp.minimum(a, b) for a, b in zip(right, left)]


def lane_gather(table, index):
    dims = lax.GatherDimensionNumbers(
        offset_dims=(),
        collapsed_slice_dims=(1,),
        start_index_map=(1,),
        operand_batching_dims=(0,),
        start_indices_batching_dims=(0,),
    )
    mode = lax.GatherScatterMode.PROMISE_IN_BOUNDS
    return lax.gather(table, index[..., None], dims, (1, 1), mode=mode)


def row(zp, y):
    return zp * PR + 8 + y


def kernel(
    dist_hbm, par_hbm, occ_hbm, rem_hbm, out, share_ref,
    dist, par, occ, field, once, snd, hal, zhal, csnd, chal, tally, theirs, rem,
    rem_sem, in_sem, ys_sem, yr_sem, zs_sem, zr_sem, cs_sem, cr_sem, ts_sem, tr_sem,
):
    gz, gy = lax.axis_index("gz"), lax.axis_index("gy")
    zc = gy % 4
    lo, hi = (gz, (gy + NGY - 1) % NGY), (gz, (gy + 1) % NGY)
    below, above = (gz + NGZ - 1) % NGZ, (gz + 1) % NGZ
    yc, half = gy // 8, (gy // 4) % 2
    stage = [
        [((gz + r) % 4, (yc * 2 + (half + h) % 2) * 4 + zc) for h in range(2) for r in range(4) if h or r],
        [(gz, (gy // 4) * 4 + (zc + r) % 4) for r in range(1, 4)],
        [(gz, (((yc + r) % 4) * 2 + half) * 4 + zc) for r in range(1, 4)],
    ]
    first_slot = (0, 7, 10)
    friends = [lo, hi, (below, gy), (above, gy)] + stage[0] + stage[1] + stage[2]

    barrier = pltpu.get_barrier_semaphore()
    for friend in friends:
        pl.semaphore_signal(barrier, inc=1, device_id=friend, device_id_type=MESH)

    fetch_removed = pltpu.make_async_copy(rem_hbm, rem, rem_sem)
    fetch_removed.start()

    def fetch(c):
        a, n = SPLIT[c], SPLIT[c + 1] - SPLIT[c]
        return [
            pltpu.make_async_copy(src.at[pl.ds(a, n)], dst.at[pl.ds(a, n)], in_sem.at[i, c])
            for i, (src, dst) in enumerate(((dist_hbm, dist), (par_hbm, par), (occ_hbm, occ)))
        ]

    for c in UNITS:
        for copy in fetch(c):
            copy.start()

    lane = lax.broadcasted_iota(jnp.int32, (8, 128), 1)
    far_tile = jnp.full((8, 128), FAR, jnp.float32)

    fetch_removed.wait()
    bits = rem[...] << lax.broadcasted_iota(jnp.int32, (32, 128), 0)
    words = jnp.broadcast_to(jnp.sum(bits, axis=0, keepdims=True), (8, 128))

    def pad_plane(zp, _):
        for xt in range(XT):
            base = pl.multiple_of(xt * RR + zp * PR, 8)
            field[pl.ds(base, 8), :] = far_tile
            once[pl.ds(base, 8), :] = far_tile
        return 0

    lax.fori_loop(0, Z + 2, pad_plane, 0)
    for xt in range(XT):
        for zp in (0, Z + 1):
            for half in (8, 16):
                field[pl.ds(xt * RR + zp * PR + half, 8), :] = far_tile
                once[pl.ds(xt * RR + zp * PR + half, 8), :] = far_tile
    for side in range(2):
        for plane in range(2):
            for xt in range(XT):
                zhal[side, plane, xt, pl.ds(0, 8), :] = far_tile
                zhal[side, plane, xt, pl.ds(24, 8), :] = far_tile

    def raise_plane(z, acc):
        for yt in range(2):
            for xt in range(XT):
                at = (z, pl.ds(yt * 8, 8), pl.ds(xt * 128, 128))
                ids, busy = par[at], occ[at]
                word = lane_gather(words, ids & 127)
                gone = lax.shift_right_logical(word, ids >> 7) & (1 - busy)
                raised = jnp.where(gone == 1, TRUNC, dist[at])
                raised = jnp.where(busy == 1, 0.0, raised)
                field[pl.ds(pl.multiple_of(xt * RR + (z + 1) * PR + 8 + yt * 8, 8), 8), :] = raised
                acc = acc + gone
        return acc

    def pack(c):
        first = c * CH + 1
        for side in range(2):
            y1, y2 = ((0, 1), (15, 14))[side]

            def rows(zp, y, xt):
                return field[pl.ds(xt * RR + row(zp, y), CH, stride=PR), :]

            near = [rows(first, y1, xt) for xt in range(XT)]
            around = lane_shifts(near, lane)
            for xt in range(XT):
                two = jnp.minimum(around[xt], rows(first, y2, xt))
                two = jnp.minimum(two, jnp.minimum(rows(first - 1, y1, xt), rows(first + 1, y1, xt)))
                snd[side, c, 0, xt] = jnp.minimum(near[xt] + VOXEL, two + VOXEL + VOXEL)
                snd[side, c, 1, xt] = near[xt] + VOXEL + VOXEL

    def y_copy(side, c):
        return pltpu.make_async_remote_copy(
            src_ref=snd.at[side, c], dst_ref=hal.at[1 - side, c],
            send_sem=ys_sem.at[side, c], recv_sem=yr_sem.at[1 - side, c],
            device_id=(lo, hi)[side], device_id_type=MESH,
        )

    def y_send(c):
        for side in (1, 0):
            y_copy(side, c).start()

    def z_copy(side, plane):
        zp = ((1, 2), (Z, Z - 1))[side][plane]
        return [
            pltpu.make_async_remote_copy(
                src_ref=field.at[pl.ds(xt * RR + row(zp, 0), 16)],
                dst_ref=zhal.at[1 - side, plane, xt, pl.ds(8, 16)],
                send_sem=zs_sem.at[side, plane, xt], recv_sem=zr_sem.at[1 - side, plane, xt],
                device_id=((below, gy), (above, gy))[side], device_id_type=MESH,
            )
            for xt in range(XT)
        ]

    def corner_copy(zs, ys):
        return pltpu.make_async_remote_copy(
            src_ref=csnd.at[zs, ys], dst_ref=chal.at[1 - zs, ys],
            send_sem=cs_sem.at[zs, ys], recv_sem=cr_sem.at[1 - zs, ys],
            device_id=((below, gy), (above, gy))[zs], device_id_type=MESH,
        )

    def z_copies(side):
        return z_copy(side, 0) + z_copy(side, 1)

    def corners(side):
        return [corner_copy(side, 0), corner_copy(side, 1)]

    has = (gz > 0, gz < NGZ - 1)

    def z_send(side):
        @pl.when(has[side])
        def _():
            for copy in z_copies(side):
                copy.start()

    def corner_send(side):
        for ys in range(2):
            for xt in range(XT):
                edge = hal[ys, (0, NC - 1)[side], 1, xt, pl.ds((0, CH - 1)[side], 1), :]
                csnd[side, ys, pl.ds(xt, 1), :] = edge

        @pl.when(has[side])
        def _():
            for copy in corners(side):
                copy.start()

    def tally_copies(s):
        return [
            pltpu.make_async_remote_copy(
                src_ref=tally.at[s], dst_ref=theirs.at[first_slot[s] + r],
                send_sem=ts_sem.at[first_slot[s] + r], recv_sem=tr_sem.at[first_slot[s] + r],
                device_id=peer, device_id_type=MESH,
            )
            for r, peer in enumerate(stage[s])
        ]

    def tally_send(s, value):
        tally[s] = value
        for copy in tally_copies(s):
            copy.start()

    def tally_wait(s, value):
        for r, copy in enumerate(tally_copies(s)):
            copy.wait()
            value = value + theirs[first_slot[s] + r]
        return value

    def sweep_chunk(src, store, c):
        def plane(z, _):
            for yt in range(2):
                base = [xt * RR + (z + 1) * PR + 8 + yt * 8 for xt in range(XT)]
                here = [src[pl.ds(pl.multiple_of(b, 8), 8), :] for b in base]
                around = lane_shifts(here, lane)
                for xt in range(XT):
                    b = base[xt]
                    m = jnp.minimum(
                        src[pl.ds(pl.multiple_of(b - PR, 8), 8), :],
                        src[pl.ds(pl.multiple_of(b + PR, 8), 8), :],
                    )
                    m = jnp.minimum(m, jnp.minimum(src[pl.ds(b - 1, 8), :], src[pl.ds(b + 1, 8), :]))
                    m = jnp.minimum(m, around[xt])
                    store(z, yt, xt, jnp.minimum(here[xt], m + VOXEL))
            return 0

        lax.fori_loop(c * CH, (c + 1) * CH, plane, 0, unroll=8)

    def store_once(z, yt, xt, value):
        once[pl.ds(pl.multiple_of(xt * RR + (z + 1) * PR + 8 + yt * 8, 8), 8), :] = value

    def out_row(z, yt, xt):
        return ((z * 2 + yt) * XT + xt) * 8

    def store_out(z, yt, xt, value):
        out[pl.ds(pl.multiple_of(out_row(z, yt, xt), 8), 8), :] = value

    acc = jnp.zeros((8, 128), jnp.int32)
    for turn, u in enumerate(UNITS):
        for copy in fetch(u):
            copy.wait()
        acc = lax.fori_loop(SPLIT[u], SPLIT[u + 1], raise_plane, acc, unroll=8)
        for c in READY[turn]:
            pack(c)
        if turn == WAIT_AT:
            pl.semaphore_wait(barrier, len(friends))
        if turn >= WAIT_AT:
            for c in EARLY[turn]:
                y_send(c)
    tally_send(0, acc)
    y_send(3)
    y_send(4)

    for c in range(NC):
        sweep_chunk(field, store_once, c)
        if c == 3:
            y_send(5)
        if c == 7:
            y_send(6)
    for c in range(NC):
        sweep_chunk(once, store_out, c)
        if c == 6:
            z_send(0)
            z_send(1)

    def y_add(c):
        for side in range(2):
            y_copy(1 - side, c).wait()
            for which in range(2):
                y = ((0, 1), (15, 14))[side][which]
                for xt in range(XT):
                    at = pl.ds(out_row(c * CH, y // 8, xt) + y % 8, CH, stride=2 * XT * 8)
                    out[at, :] = jnp.minimum(out[at, :], hal[side, c, which, xt])

    for c in ORDER[:2]:
        y_add(c)
    corner_send(0)
    corner_send(1)
    acc = tally_wait(0, acc)
    tally_send(1, acc)

    for side in range(2):
        z0, z1 = ((0, 1), (Z - 1, Z - 2))[side]

        @pl.when(has[side])
        def _():
            for sent, came in zip(z_copies(side) + corners(side), z_copies(1 - side) + corners(1 - side)):
                sent.wait_send()
                came.wait_recv()
            for yt in range(2):
                near = [zhal[side, 0, xt, pl.ds(8 + yt * 8, 8), :] for xt in range(XT)]
                around = lane_shifts(near, lane)
                for xt in range(XT):
                    two = jnp.minimum(around[xt], zhal[side, 1, xt, pl.ds(8 + yt * 8, 8), :])
                    two = jnp.minimum(
                        two,
                        jnp.minimum(
                            zhal[side, 0, xt, pl.ds(7 + yt * 8, 8), :],
                            zhal[side, 0, xt, pl.ds(9 + yt * 8, 8), :],
                        ),
                    )
                    add0 = jnp.minimum(near[xt] + VOXEL, two + VOXEL + VOXEL)
                    at0 = pl.ds(out_row(z0, yt, xt), 8)
                    out[at0, :] = jnp.minimum(out[at0, :], add0)
                    at1 = pl.ds(out_row(z1, yt, xt), 8)
                    out[at1, :] = jnp.minimum(out[at1, :], near[xt] + VOXEL + VOXEL)
            for ys in range(2):
                at = pl.ds(out_row(z0, ys, 0) + (0, 7)[ys], 8, stride=8)
                out[at, :] = jnp.minimum(out[at, :], chal[side, ys])

    for c in ORDER[2:]:
        y_add(c)
        if c == 4:
            acc = tally_wait(1, acc)
            tally_send(2, acc)

    acc = tally_wait(2, acc)
    count = jnp.sum(acc)
    share_ref[0, 0] = count.astype(jnp.float32) * jnp.float32(100.0 / (NGZ * Z * NGY * Y * X))


def on_device(distance, parent, removed, occupied):
    hbm = pl.BlockSpec(memory_space=pltpu.HBM)
    vmem = pl.BlockSpec(memory_space=pltpu.VMEM)
    dma = pltpu.SemaphoreType.DMA
    flat, share = pl.pallas_call(
        kernel,
        out_shape=(
            jax.ShapeDtypeStruct((Z * Y * XT, 128), jnp.float32),
            jax.ShapeDtypeStruct((1, 1), jnp.float32),
        ),
        in_specs=[hbm, hbm, hbm, hbm],
        out_specs=(vmem, pl.BlockSpec(memory_space=pltpu.SMEM)),
        scratch_shapes=[
            pltpu.VMEM((Z, Y, X), jnp.float32),
            pltpu.VMEM((Z, Y, X), jnp.int32),
            pltpu.VMEM((Z, Y, X), jnp.int32),
            pltpu.VMEM((XT * RR, 128), jnp.float32),
            pltpu.VMEM((XT * RR, 128), jnp.float32),
            pltpu.VMEM((2, NC, 2, XT, CH, 128), jnp.float32),
            pltpu.VMEM((2, NC, 2, XT, CH, 128), jnp.float32),
            pltpu.VMEM((2, 2, XT, 32, 128), jnp.float32),
            pltpu.VMEM((2, 2, 8, 128), jnp.float32),
            pltpu.VMEM((2, 2, 8, 128), jnp.float32),
            pltpu.VMEM((3, 8, 128), jnp.int32),
            pltpu.VMEM((13, 8, 128), jnp.int32),
            pltpu.VMEM((32, 128), jnp.int32),
            dma,
            dma((3, NC)),
            dma((2, NC)),
            dma((2, NC)),
            dma((2, 2, XT)),
            dma((2, 2, XT)),
            dma((2, 2)),
            dma((2, 2)),
            dma((13,)),
            dma((13,)),
        ],
        compiler_params=pltpu.CompilerParams(
            collective_id=0, has_side_effects=True, vmem_limit_bytes=48 * 2**20
        ),
    )(distance, parent, occupied, removed.reshape(32, 128))
    lowered = flat.reshape(Z, 2, XT, 8, 128).transpose(0, 1, 3, 2, 4).reshape(Z, Y, X)
    return lowered, share.reshape(())


def solution(mesh):
    block = P("gz", "gy", None)
    return jax.shard_map(
        on_device, mesh=mesh, in_specs=(block, block, P(), block), out_specs=(block, P()), check_vma=False
    )
```

```python
import functools

import jax
import jax.numpy as jnp
from jax import lax
from jax.experimental import pallas as pl
from jax.experimental.pallas import tpu as pltpu
from jax.sharding import PartitionSpec as P

MESH = pl.DeviceIdType.MESH
FAR = 1000000.0
VOXEL = 0.1
TRUNC = 2.0
Z, Y, X = 64, 16, 1024
XT = X // 128
PR = 24
RR = (Z + 2) * PR
CH = 8
NC = Z // CH
NGZ, NGY = 4, 32
WAIT_AT = 1
UNITS = (0, 7, 6, 1, 2, 3, 4, 5)
READY = ((0,), (), (7,), (1,), (2,), (3,), (4,), (5, 6))
EARLY = ((), (0,), (7,), (1,), (2,), (), (), ())
ORDER = (0, 7, 1, 2, 3, 4, 5, 6)
SPLIT = (0,) + tuple(CH * c + CH + 1 for c in range(NC - 1)) + (Z,)


def lane_shifts(tiles, lane):
    far = jnp.full((8, 128), FAR, jnp.float32)
    up = [pltpu.roll(t, 127, 1) for t in tiles] + [far]
    down = [far] + [pltpu.roll(t, 1, 1) for t in tiles]
    right = [jnp.where(lane == 127, up[i + 1], up[i]) for i in range(len(tiles))]
    left = [jnp.where(lane == 0, down[i], down[i + 1]) for i in range(len(tiles))]
    return [jnp.minimum(a, b) for a, b in zip(right, left)]


def lane_gather(table, index):
    dims = lax.GatherDimensionNumbers(
        offset_dims=(),
        collapsed_slice_dims=(1,),
        start_index_map=(1,),
        operand_batching_dims=(0,),
        start_indices_batching_dims=(0,),
    )
    mode = lax.GatherScatterMode.PROMISE_IN_BOUNDS
    return lax.gather(table, index[..., None], dims, (1, 1), mode=mode)


def row(zp, y):
    return zp * PR + 8 + y


def kernel(
    dist_hbm, par_hbm, occ_hbm, rem_ref, out, share_ref,
    dist, par, occ, field, once, snd, hal, zhal, csnd, chal, tally, theirs,
    in_sem, ys_sem, yr_sem, zs_sem, zr_sem, cs_sem, cr_sem, ts_sem, tr_sem,
):
    gz, gy = lax.axis_index("gz"), lax.axis_index("gy")
    zc = gy % 4
    lo, hi = (gz, (gy + NGY - 1) % NGY), (gz, (gy + 1) % NGY)
    below, above = (gz + NGZ - 1) % NGZ, (gz + 1) % NGZ
    yc, half = gy // 8, (gy // 4) % 2
    stage = [
        [((gz + r) % 4, (yc * 2 + (half + h) % 2) * 4 + zc) for h in range(2) for r in range(4) if h or r],
        [(gz, (gy // 4) * 4 + (zc + r) % 4) for r in range(1, 4)],
        [(gz, (((yc + r) % 4) * 2 + half) * 4 + zc) for r in range(1, 4)],
    ]
    first_slot = (0, 7, 10)
    friends = [lo, hi, (below, gy), (above, gy)] + stage[0] + stage[1] + stage[2]

    barrier = pltpu.get_barrier_semaphore()
    for friend in friends:
        pl.semaphore_signal(barrier, inc=1, device_id=friend, device_id_type=MESH)

    def fetch(c):
        a, n = SPLIT[c], SPLIT[c + 1] - SPLIT[c]
        return [
            pltpu.make_async_copy(src.at[pl.ds(a, n)], dst.at[pl.ds(a, n)], in_sem.at[i, c])
            for i, (src, dst) in enumerate(((dist_hbm, dist), (par_hbm, par), (occ_hbm, occ)))
        ]

    for c in UNITS:
        for copy in fetch(c):
            copy.start()

    lane = lax.broadcasted_iota(jnp.int32, (8, 128), 1)
    far_tile = jnp.full((8, 128), FAR, jnp.float32)

    bits = rem_ref[...] << lax.broadcasted_iota(jnp.int32, (32, 128), 0)
    words = jnp.broadcast_to(jnp.sum(bits, axis=0, keepdims=True), (8, 128))

    def pad_plane(zp, _):
        for xt in range(XT):
            base = pl.multiple_of(xt * RR + zp * PR, 8)
            field[pl.ds(base, 8), :] = far_tile
            once[pl.ds(base, 8), :] = far_tile
        return 0

    lax.fori_loop(0, Z + 2, pad_plane, 0)
    for xt in range(XT):
        for zp in (0, Z + 1):
            for half in (8, 16):
                field[pl.ds(xt * RR + zp * PR + half, 8), :] = far_tile
                once[pl.ds(xt * RR + zp * PR + half, 8), :] = far_tile
    for side in range(2):
        for plane in range(2):
            for xt in range(XT):
                zhal[side, plane, xt, pl.ds(0, 8), :] = far_tile
                zhal[side, plane, xt, pl.ds(24, 8), :] = far_tile

    def raise_plane(z, acc):
        for yt in range(2):
            for xt in range(XT):
                at = (z, pl.ds(yt * 8, 8), pl.ds(xt * 128, 128))
                ids, busy = par[at], occ[at]
                word = lane_gather(words, ids & 127)
                gone = lax.shift_right_logical(word, ids >> 7) & (1 - busy)
                raised = jnp.where(gone == 1, TRUNC, dist[at])
                raised = jnp.where(busy == 1, 0.0, raised)
                field[pl.ds(pl.multiple_of(xt * RR + (z + 1) * PR + 8 + yt * 8, 8), 8), :] = raised
                acc = acc + gone
        return acc

    def pack(c):
        first = c * CH + 1
        for side in range(2):
            y1, y2 = ((0, 1), (15, 14))[side]

            def rows(zp, y, xt):
                return field[pl.ds(xt * RR + row(zp, y), CH, stride=PR), :]

            near = [rows(first, y1, xt) for xt in range(XT)]
            around = lane_shifts(near, lane)
            for xt in range(XT):
                two = jnp.minimum(around[xt], rows(first, y2, xt))
                two = jnp.minimum(two, jnp.minimum(rows(first - 1, y1, xt), rows(first + 1, y1, xt)))
                snd[side, c, 0, xt] = jnp.minimum(near[xt] + VOXEL, two + VOXEL + VOXEL)
                snd[side, c, 1, xt] = near[xt] + VOXEL + VOXEL

    def y_copy(side, c):
        return pltpu.make_async_remote_copy(
            src_ref=snd.at[side, c], dst_ref=hal.at[1 - side, c],
            send_sem=ys_sem.at[side, c], recv_sem=yr_sem.at[1 - side, c],
            device_id=(lo, hi)[side], device_id_type=MESH,
        )

    def y_send(c):
        for side in (1, 0):
            y_copy(side, c).start()

    def z_copy(side, plane):
        zp = ((1, 2), (Z, Z - 1))[side][plane]
        return [
            pltpu.make_async_remote_copy(
                src_ref=field.at[pl.ds(xt * RR + row(zp, 0), 16)],
                dst_ref=zhal.at[1 - side, plane, xt, pl.ds(8, 16)],
                send_sem=zs_sem.at[side, plane, xt], recv_sem=zr_sem.at[1 - side, plane, xt],
                device_id=((below, gy), (above, gy))[side], device_id_type=MESH,
            )
            for xt in range(XT)
        ]

    def corner_copy(zs, ys):
        return pltpu.make_async_remote_copy(
            src_ref=csnd.at[zs, ys], dst_ref=chal.at[1 - zs, ys],
            send_sem=cs_sem.at[zs, ys], recv_sem=cr_sem.at[1 - zs, ys],
            device_id=((below, gy), (above, gy))[zs], device_id_type=MESH,
        )

    def z_copies(side):
        return z_copy(side, 0) + z_copy(side, 1)

    def corners(side):
        return [corner_copy(side, 0), corner_copy(side, 1)]

    has = (gz > 0, gz < NGZ - 1)

    def z_send(side):
        @pl.when(has[side])
        def _():
            for copy in z_copies(side):
                copy.start()

    def corner_send(side):
        for ys in range(2):
            for xt in range(XT):
                edge = hal[ys, (0, NC - 1)[side], 1, xt, pl.ds((0, CH - 1)[side], 1), :]
                csnd[side, ys, pl.ds(xt, 1), :] = edge

        @pl.when(has[side])
        def _():
            for copy in corners(side):
                copy.start()

    def tally_copies(s):
        return [
            pltpu.make_async_remote_copy(
                src_ref=tally.at[s], dst_ref=theirs.at[first_slot[s] + r],
                send_sem=ts_sem.at[first_slot[s] + r], recv_sem=tr_sem.at[first_slot[s] + r],
                device_id=peer, device_id_type=MESH,
            )
            for r, peer in enumerate(stage[s])
        ]

    def tally_send(s, value):
        tally[s] = value
        for copy in tally_copies(s):
            copy.start()

    def tally_wait(s, value):
        for r, copy in enumerate(tally_copies(s)):
            copy.wait()
            value = value + theirs[first_slot[s] + r]
        return value

    def sweep_chunk(src, store, c):
        def plane(z, _):
            for yt in range(2):
                base = [xt * RR + (z + 1) * PR + 8 + yt * 8 for xt in range(XT)]
                here = [src[pl.ds(pl.multiple_of(b, 8), 8), :] for b in base]
                around = lane_shifts(here, lane)
                for xt in range(XT):
                    b = base[xt]
                    m = jnp.minimum(
                        src[pl.ds(pl.multiple_of(b - PR, 8), 8), :],
                        src[pl.ds(pl.multiple_of(b + PR, 8), 8), :],
                    )
                    m = jnp.minimum(m, jnp.minimum(src[pl.ds(b - 1, 8), :], src[pl.ds(b + 1, 8), :]))
                    m = jnp.minimum(m, around[xt])
                    store(z, yt, xt, jnp.minimum(here[xt], m + VOXEL))
            return 0

        lax.fori_loop(c * CH, (c + 1) * CH, plane, 0, unroll=8)

    def store_once(z, yt, xt, value):
        once[pl.ds(pl.multiple_of(xt * RR + (z + 1) * PR + 8 + yt * 8, 8), 8), :] = value

    def out_row(z, yt, xt):
        return ((z * 2 + yt) * XT + xt) * 8

    def store_out(z, yt, xt, value):
        out[pl.ds(pl.multiple_of(out_row(z, yt, xt), 8), 8), :] = value

    acc = jnp.zeros((8, 128), jnp.int32)
    for turn, u in enumerate(UNITS):
        for copy in fetch(u):
            copy.wait()
        acc = lax.fori_loop(SPLIT[u], SPLIT[u + 1], raise_plane, acc, unroll=8)
        for c in READY[turn]:
            pack(c)
        if turn == WAIT_AT:
            pl.semaphore_wait(barrier, len(friends))
        if turn >= WAIT_AT:
            for c in EARLY[turn]:
                y_send(c)
    tally_send(0, acc)
    y_send(3)
    y_send(4)

    for c in range(NC):
        sweep_chunk(field, store_once, c)
        if c == 3:
            y_send(5)
        if c == 7:
            y_send(6)
    for c in range(NC):
        sweep_chunk(once, store_out, c)
        if c == 6:
            z_send(0)
            z_send(1)

    def y_add(c):
        for side in range(2):
            y_copy(1 - side, c).wait()
            for which in range(2):
                y = ((0, 1), (15, 14))[side][which]
                for xt in range(XT):
                    at = pl.ds(out_row(c * CH, y // 8, xt) + y % 8, CH, stride=2 * XT * 8)
                    out[at, :] = jnp.minimum(out[at, :], hal[side, c, which, xt])

    y_add(ORDER[0])
    acc = tally_wait(0, acc)
    tally_send(1, acc)
    y_add(ORDER[1])
    corner_send(0)
    corner_send(1)

    for c in ORDER[2:]:
        y_add(c)
        if c == 2:
            acc = tally_wait(1, acc)
            tally_send(2, acc)

    for side in range(2):
        z0, z1 = ((0, 1), (Z - 1, Z - 2))[side]

        @pl.when(has[side])
        def _():
            for sent, came in zip(z_copies(side) + corners(side), z_copies(1 - side) + corners(1 - side)):
                sent.wait_send()
                came.wait_recv()
            for yt in range(2):
                near = [zhal[side, 0, xt, pl.ds(8 + yt * 8, 8), :] for xt in range(XT)]
                around = lane_shifts(near, lane)
                for xt in range(XT):
                    two = jnp.minimum(around[xt], zhal[side, 1, xt, pl.ds(8 + yt * 8, 8), :])
                    two = jnp.minimum(
                        two,
                        jnp.minimum(
                            zhal[side, 0, xt, pl.ds(7 + yt * 8, 8), :],
                            zhal[side, 0, xt, pl.ds(9 + yt * 8, 8), :],
                        ),
                    )
                    add0 = jnp.minimum(near[xt] + VOXEL, two + VOXEL + VOXEL)
                    at0 = pl.ds(out_row(z0, yt, xt), 8)
                    out[at0, :] = jnp.minimum(out[at0, :], add0)
                    at1 = pl.ds(out_row(z1, yt, xt), 8)
                    out[at1, :] = jnp.minimum(out[at1, :], near[xt] + VOXEL + VOXEL)
            for ys in range(2):
                at = pl.ds(out_row(z0, ys, 0) + (0, 7)[ys], 8, stride=8)
                out[at, :] = jnp.minimum(out[at, :], chal[side, ys])

    acc = tally_wait(2, acc)
    count = jnp.sum(acc)
    share_ref[0, 0] = count.astype(jnp.float32) * jnp.float32(100.0 / (NGZ * Z * NGY * Y * X))


def on_device(distance, parent, removed, occupied):
    hbm = pl.BlockSpec(memory_space=pltpu.HBM)
    vmem = pl.BlockSpec(memory_space=pltpu.VMEM)
    dma = pltpu.SemaphoreType.DMA
    flat, share = pl.pallas_call(
        kernel,
        out_shape=(
            jax.ShapeDtypeStruct((Z * Y * XT, 128), jnp.float32),
            jax.ShapeDtypeStruct((1, 1), jnp.float32),
        ),
        in_specs=[hbm, hbm, hbm, vmem],
        out_specs=(vmem, pl.BlockSpec(memory_space=pltpu.SMEM)),
        scratch_shapes=[
            pltpu.VMEM((Z, Y, X), jnp.float32),
            pltpu.VMEM((Z, Y, X), jnp.int32),
            pltpu.VMEM((Z, Y, X), jnp.int32),
            pltpu.VMEM((XT * RR, 128), jnp.float32),
            pltpu.VMEM((XT * RR, 128), jnp.float32),
            pltpu.VMEM((2, NC, 2, XT, CH, 128), jnp.float32),
            pltpu.VMEM((2, NC, 2, XT, CH, 128), jnp.float32),
            pltpu.VMEM((2, 2, XT, 32, 128), jnp.float32),
            pltpu.VMEM((2, 2, 8, 128), jnp.float32),
            pltpu.VMEM((2, 2, 8, 128), jnp.float32),
            pltpu.VMEM((3, 8, 128), jnp.int32),
            pltpu.VMEM((13, 8, 128), jnp.int32),
            dma((3, NC)),
            dma((2, NC)),
            dma((2, NC)),
            dma((2, 2, XT)),
            dma((2, 2, XT)),
            dma((2, 2)),
            dma((2, 2)),
            dma((13,)),
            dma((13,)),
        ],
        compiler_params=pltpu.CompilerParams(
            collective_id=0, has_side_effects=True, vmem_limit_bytes=48 * 2**20
        ),
    )(distance, parent, occupied, removed.reshape(32, 128))
    lowered = flat.reshape(Z, 2, XT, 8, 128).transpose(0, 1, 3, 2, 4).reshape(Z, Y, X)
    return lowered, share.reshape(())


def solution(mesh):
    block = P("gz", "gy", None)
    return jax.shard_map(
        on_device, mesh=mesh, in_specs=(block, block, P(), block), out_specs=(block, P()), check_vma=False
    )
```
